128 devices in a mesh: vert: 32 (over x, y, core), feat: 4 (over z).
Axes of the slice: x: 4, y: 4, z: 4, core: 2. Of those that a mesh axis runs over, the one named last changes fastest.
Arguments:
- features: bfloat16 [256, 262144], P('feat', 'vert'), may hold values from -6 to 6
- tile_vals: bfloat16 [16384, 128, 128], P('vert'), may hold values from -0.1875 to 0.1875
- tile_row: int32 [32, 512], P('vert'), may hold values from 0 to 63
- tile_col: int32 [32, 512], P('vert'), may hold values from 0 to 95
- tile_count: int32 [32], P('vert'), may hold values from 1 to 512, as said below
- recv_rows: int32 [32, 32, 128], P('vert'), may hold values from 0 to 8191
- recv_count: int32 [32, 32], P('vert'), may hold values from 0 to 128, as said below
- weight: bfloat16 [256, 256], replicated, may hold values from -0.375 to 0.375
- bias: float32 [256], replicated, may hold values from -4 to 4
Outputs:
- layer_out: bfloat16 [262144, 256], P(('vert', 'feat'))
The draws below stay inside these ranges and needn't reach their ends.
Inputs may be any that keep to these rules, and one draw needn't show every extreme that they name: `tile_count`: tile slots at or past a partition's count are padding with arbitrary contents; some partition uses all 512 slots. `recv_count`: slots at or past the count hold arbitrary valid vertices; some pair uses all 128 slots.
All inputs are finite; a program needn't handle non-finite values.
Results may differ from the reference program's by a relative error of at most 0.0075.
Values may be sent and summed in bfloat16 or wider, within the bound.
No kernel may reach another device: no remote copies, remote signals or barrier semaphores. Data moves between devices by JAX's collectives and lax.ppermute only.
A program may use at most 256 MiB of HBM per device.

```python
import jax
import jax.numpy as jnp
from jax import lax

FIN = 256
FOUT = 256
BLOCK = 128
V_DEV = 8192
TILES = 512
SLOT = 128
NODES = 262144
NCOLB = 96
N_VERT = 32


def draw_tile_count(key, part):
    first, second = jax.random.split(jax.random.fold_in(key, 11))
    counts = jax.random.randint(first, (N_VERT,), max(1, TILES // 4), max(2, TILES // 2 + 1))
    chosen = jax.random.randint(second, (), 0, N_VERT)
    return jnp.where(jnp.arange(N_VERT) == chosen, TILES, counts).astype(jnp.int32)


def draw_recv_count(key, part):
    first, second = jax.random.split(jax.random.fold_in(key, 23))
    counts = jax.random.randint(first, (N_VERT, N_VERT), 0, SLOT + 1)
    chosen = jax.random.randint(second, (), 0, N_VERT * N_VERT)
    flat = jnp.where(jnp.arange(N_VERT * N_VERT) == chosen, SLOT, counts.reshape(-1))
    return flat.reshape(N_VERT, N_VERT).astype(jnp.int32)


def set_ends(entries, own_key, least, largest):
    longest = entries.shape.index(max(entries.shape))
    spots = []
    for shift in (0, 1):
        where = [jax.random.randint(jax.random.fold_in(own_key, axis), (), 0, length) for axis, length in enumerate(entries.shape)]
        where[longest] = (where[longest] + shift) % entries.shape[longest]
        spots.append(tuple(where))
    return entries.at[spots[0]].set(least).at[spots[1]].set(largest)


def shard_levels(rng, dims, cuts, smallest, largest):
    def one(position, blocks):
        draws = jax.random.uniform(jax.random.fold_in(jax.random.fold_in(rng, 6), position), (blocks,), jnp.float32, smallest / len(cuts), largest / len(cuts))
        return jnp.repeat(jnp.exp(draws), dims[position] // blocks).reshape((-1,) + (1,) * (len(dims) - position - 1))

    level = one(*cuts[0])
    for cut in cuts[1:]:
        level = level * one(*cut)
    return level


def gaussian(rng, extent, width, most, pieces=(), held_as=jnp.bfloat16):
    factor_of = shard_levels(rng, extent, pieces, -0.22, 0.18) if pieces else 1.0
    result = jax.random.normal(rng, extent, jnp.float32) * width * factor_of
    return jnp.minimum(jnp.maximum(result, -most), most).astype(held_as)


def setup_inputs(seed: int = 0) -> dict:
    arg_keys = jax.random.split(jax.random.key(seed), 10)
    return {
        "features": gaussian(arg_keys[0], (FIN, NODES), 1.0, 6.0, ((0, 4), (1, 32))),
        "tile_vals": gaussian(arg_keys[1], (N_VERT * TILES, BLOCK, BLOCK), (BLOCK * TILES * BLOCK // V_DEV) ** -0.5, 0.1875, ((0, 32),)),
        "tile_row": set_ends(jax.random.randint(arg_keys[2], (N_VERT, TILES), 0, V_DEV // BLOCK), jax.random.fold_in(arg_keys[2], 1), 0, (V_DEV // BLOCK) - 1).astype(jnp.int32),
        "tile_col": set_ends(jax.random.randint(arg_keys[3], (N_VERT, TILES), 0, NCOLB), jax.random.fold_in(arg_keys[3], 1), 0, NCOLB - 1).astype(jnp.int32),
        "tile_count": draw_tile_count(jax.random.fold_in(arg_keys[9], 71), 0),
        "recv_rows": set_ends(jax.random.randint(arg_keys[5], (N_VERT, N_VERT, SLOT), 0, V_DEV), jax.random.fold_in(arg_keys[5], 1), 0, V_DEV - 1).astype(jnp.int32),
        "recv_count": draw_recv_count(jax.random.fold_in(arg_keys[9], 71), 0),
        "weight": gaussian(arg_keys[7], (FIN, FOUT), FIN ** -0.5, 0.375),
        "bias": gaussian(arg_keys[8], (FOUT,), 1.0, 4.0, (), jnp.float32),
    }


def one_partition(args, flat_rows):
    local, vals, rows_blk, cols_blk, count, asked, asked_count = args
    owners = jnp.arange(N_VERT, dtype=jnp.int32)[:, None] * V_DEV
    index = (owners + asked.astype(jnp.int32)).reshape(-1)
    remote = flat_rows[index].reshape(N_VERT, SLOT, FIN)
    usable = jnp.arange(SLOT, dtype=jnp.int32)[None, :] < asked_count[:, None]
    remote = jnp.where(usable[:, :, None], remote, jnp.zeros_like(remote))
    rowbuf = jnp.concatenate([local, remote.reshape(N_VERT * SLOT, FIN)], axis=0)
    blocks = rowbuf.reshape(NCOLB, BLOCK, FIN)[cols_blk]
    product = jnp.einsum("tij,tjf->tif", vals.astype(jnp.float32), blocks.astype(jnp.float32), precision=lax.Precision.HIGHEST)
    used = (jnp.arange(TILES, dtype=jnp.int32) < count).astype(jnp.float32)
    onehot = (rows_blk[None, :] == jnp.arange(V_DEV // BLOCK, dtype=jnp.int32)[:, None]).astype(jnp.float32) * used[None, :]
    aggregate = jnp.einsum("rt,tif->rif", onehot, product, precision=lax.Precision.HIGHEST)
    return aggregate.reshape(V_DEV, FIN).astype(jnp.bfloat16)


def reference(features, tile_vals, tile_row, tile_col, tile_count, recv_rows, recv_count, weight, bias):
    flat_rows = features.T
    per_part = (flat_rows.reshape(N_VERT, V_DEV, FIN), tile_vals.reshape(N_VERT, TILES, BLOCK, BLOCK), tile_row, tile_col, tile_count, recv_rows, recv_count)
    aggregate = lax.map(lambda a: one_partition(a, flat_rows), per_part).reshape(N_VERT * V_DEV, FIN)
    hidden = jnp.dot(aggregate, weight, preferred_element_type=jnp.float32) + bias
    return jnp.maximum(hidden, 0.0).astype(jnp.bfloat16)
```

```python
import jax
import jax.numpy as jnp
from jax import lax
from jax.experimental import pallas as pl
from jax.experimental.pallas import tpu as pltpu
from jax.sharding import PartitionSpec as P

U = 8
DEPTH = 5
NT = (((1,), (1,)), ((), ()))
TN = (((0,), (0,)), ((), ()))
VMEM = pl.BlockSpec(memory_space=pltpu.VMEM)
HBM = pl.BlockSpec(memory_space=pltpu.HBM)
SMEM = pl.BlockSpec(memory_space=pltpu.SMEM)
BF, F32, I32 = jnp.bfloat16, jnp.float32, jnp.int32


def params(mib):
    return pltpu.CompilerParams(vmem_limit_bytes=mib << 20)


def cost(flops, nbytes):
    return pl.CostEstimate(flops=flops, bytes_accessed=nbytes, transcendentals=0)


def tile_lists(tile_row, tile_col, tile_count):
    n = tile_row.shape[0]
    t = jnp.arange(n, dtype=I32)
    far = (tile_col >= 64).astype(I32)
    key = jnp.where(t < tile_count, tile_row + 64 * far, 128)
    b = jnp.arange(128, dtype=I32)
    member = (key[None, :] == b[:, None]).astype(I32)
    pairs = (jnp.sum(member, axis=1) + 1) // 2
    before = jnp.sum(jnp.where(b[None, :] < b[:, None], pairs[None, :], 0), axis=1)
    local = jnp.sum(jnp.where(b < 64, pairs, 0))
    first = (local + U - 1) // U * U
    end = first + jnp.sum(jnp.where(b < 64, 0, pairs))
    base = before + jnp.where(b < 64, 0, first - local)
    place = jnp.sum(
        ((key[None, :] == key[:, None]) & (t[None, :] < t[:, None])).astype(I32), axis=1
    )
    slot = 2 * jnp.sum(member * base[:, None], axis=0) + place
    slot = jnp.where(key < 128, slot, -1)
    entry = t | (tile_row << 9) | ((tile_col - 64 * far + 1) << 15)
    s = jnp.arange(640 + 4 * U, dtype=I32)
    entries = jnp.sum(jnp.where(slot[None, :] == s[:, None], entry[None, :], 0), axis=1)
    return entries, jnp.stack([first, end])


def table_kernel(x_ref, out_ref):
    half = out_ref.shape[0]

    def step(k, _):
        at = pl.multiple_of(k * 128, 128)
        x = jnp.concatenate([x_ref[:, pl.ds(at, 128)], x_ref[:, pl.ds(at + half, 128)]], axis=0)
        out_ref[pl.ds(at, 128), :] = x.astype(F32).T
        return 0

    lax.fori_loop(0, half // 128, step, 0, unroll=4)


def gather_kernel(idx_ref, which_ref, table_ref, out_ref, rows_ref, buf, sem):
    half = table_ref.shape[0]

    def step(p, _):
        for s in range(128):
            rows_ref[s : s + 1, :] = table_ref[idx_ref[p, s] & (half - 1)]
        g = rows_ref[...].T
        buf[p] = jnp.where(which_ref[p] < half, g[:64], g[64:]).astype(BF)
        pltpu.make_async_copy(buf.at[p], out_ref.at[p], sem).start()
        return 0

    lax.fori_loop(0, out_ref.shape[0], step, 0)
    pltpu.make_async_copy(buf, out_ref, sem).wait()


class Tiles:
    def __init__(self, start, end, list_ref, vals_ref, buf, sems):
        self.start, self.list, self.vals, self.buf, self.sems = start, list_ref, vals_ref, buf, sems
        self.groups = (end - start + U - 1) // U

    def fetch(self, c):
        slot = lax.rem(c, DEPTH)
        for k in range(2 * U):
            e = self.list[2 * (self.start + c * U) + k]
            pltpu.make_async_copy(
                self.vals.at[e & 511], self.buf.at[slot * 2 * U + k], self.sems.at[slot]
            ).start()

    def begin(self):
        def step(c, _):
            self.fetch(c)
            return 0

        lax.fori_loop(0, jnp.minimum(self.groups, DEPTH - 1), step, 0)

    def add(self, block, acc_ref):
        def step(c, _):
            @pl.when(c + DEPTH - 1 < self.groups)
            def _():
                self.fetch(c + DEPTH - 1)

            slot = lax.rem(c, DEPTH)
            here = pl.ds(pl.multiple_of(slot * 2 * U, 2 * U), 2 * U)
            pltpu.make_async_copy(
                self.vals.at[pl.ds(0, 2 * U)], self.buf.at[here], self.sems.at[slot]
            ).wait()
            found = []
            for u in range(U):
                at = 2 * (self.start + c * U + u)
                e, f = self.list[at], self.list[at + 1]
                at = slot * 2 * U + 2 * u
                lhs = jnp.concatenate([block(e), block(f)], axis=1)
                rhs = jnp.concatenate([self.buf[at], self.buf[at + 1]], axis=1)
                found.append(
                    ((e >> 9) & 63, lax.dot_general(lhs, rhs, NT, preferred_element_type=F32))
                )
            for r, product in found:
                acc_ref[r] = acc_ref[r] + product
            return 0

        lax.fori_loop(0, self.groups, step, 0)


def local_kernel(list_ref, ends_ref, x_ref, vals_ref, acc_ref, buf, sems):
    tiles = Tiles(0, ends_ref[0], list_ref, vals_ref, buf, sems)
    tiles.begin()
    acc_ref[...] = jnp.zeros_like(acc_ref)

    def block(e):
        c = jnp.maximum((e >> 15) - 1, 0)
        x = x_ref[:, pl.ds(pl.multiple_of(c * 128, 128), 128)]
        return jnp.where(e > 0, x, jnp.zeros_like(x))

    tiles.add(block, acc_ref)


def remote_kernel(z_ref, list_ref, ends_ref, count_ref, sum_ref, far_ref, vals_ref, *rest):
    out_refs, (acc_ref, sum_buf, far_buf, sum_sem, far_sem, buf, sems) = rest[:4], rest[4:]
    parts = far_ref.shape[0]
    far_copy = pltpu.make_async_copy(far_ref, far_buf.at[pl.ds(1, parts)], far_sem)
    far_copy.start()
    tiles = Tiles(ends_ref[0], ends_ref[1], list_ref, vals_ref, buf, sems)
    tiles.begin()
    sum_copy = pltpu.make_async_copy(sum_ref, sum_buf, sum_sem)
    sum_copy.start()
    acc_ref[...] = jnp.zeros_like(acc_ref)
    far_buf[0] = jnp.zeros_like(far_buf[0])
    lane = lax.broadcasted_iota(I32, far_buf.shape[1:], 1)
    far_copy.wait()

    def clear(q, _):
        x = far_buf[q + 1]
        far_buf[q + 1] = jnp.where(lane < count_ref[q], x, jnp.zeros_like(x))
        return 0

    lax.fori_loop(0, parts, clear, 0, unroll=4)
    tiles.add(lambda e: far_buf[e >> 15], acc_ref)
    sum_copy.wait()
    z = z_ref[0]
    for k, out_ref in enumerate(out_refs):
        first = ((z + k) & 3) * 16
        for r in range(16):
            out_ref[r] = (acc_ref[first + r] + sum_buf[first + r]).astype(BF)


def project_kernel(z_ref, a_ref, b_ref, c_ref, d_ref, weight_ref, bias_ref, out_ref, w_ref):
    z = z_ref[0]
    for k in range(4):
        first = pl.multiple_of(((z - k) & 3) * 64, 64)
        w_ref[64 * k : 64 * k + 64, :] = weight_ref[pl.ds(first, 64), :]
    w = w_ref[...]
    for r in range(a_ref.shape[0]):
        x = jnp.concatenate([a_ref[r], b_ref[r], c_ref[r], d_ref[r]], axis=0)
        y = lax.dot_general(x, w, TN, preferred_element_type=F32) + bias_ref[...]
        out_ref[128 * r : 128 * r + 128, :] = jnp.maximum(y, 0.0).astype(BF)


def on_device(
    features, tile_vals, tile_row, tile_col, tile_count, recv_rows, recv_count, weight, bias
):
    width, v_rows = features.shape
    parts = recv_rows.shape[1]
    wanted = lax.all_to_all(recv_rows[0], "vert", split_axis=0, concat_axis=0, tiled=True)

    entries, ends = tile_lists(tile_row[0], tile_col[0], tile_count[0])
    table = pl.pallas_call(
        table_kernel,
        out_shape=jax.ShapeDtypeStruct((v_rows // 2, 128), F32),
        in_specs=[VMEM],
        out_specs=VMEM,
        compiler_params=params(8),
        cost_estimate=cost(10**7, 5 * 2**20),
        name="table",
    )(features)

    outgoing = pl.pallas_call(
        gather_kernel,
        out_shape=jax.ShapeDtypeStruct((parts, width, 128), BF),
        in_specs=[SMEM, VMEM, VMEM],
        out_specs=HBM,
        scratch_shapes=[
            pltpu.VMEM((128, 128), F32),
            pltpu.VMEM((parts, width, 128), BF),
            pltpu.SemaphoreType.DMA,
        ],
        compiler_params=params(57),
        cost_estimate=cost(10**7, 5 * 2**20),
        name="gather",
    )(wanted, wanted.reshape(parts, 1, 128), table.reshape(v_rows // 2, 1, 128))

    far = lax.all_to_all(outgoing, "vert", split_axis=0, concat_axis=0, tiled=True)

    acc = jax.ShapeDtypeStruct((v_rows // 128, width, 128), F32)
    ring = [pltpu.VMEM((DEPTH * 2 * U, 128, 128), BF), pltpu.SemaphoreType.DMA((DEPTH,))]
    local = pl.pallas_call(
        local_kernel,
        out_shape=acc,
        in_specs=[SMEM, SMEM, VMEM, HBM],
        out_specs=VMEM,
        scratch_shapes=ring,
        compiler_params=params(56),
        cost_estimate=cost(8 * 10**8, 20 * 2**20),
        name="local_tiles",
    )(entries, ends, features, tile_vals)

    z = lax.axis_index("feat").astype(I32)[None]
    piece = jax.ShapeDtypeStruct((16, width, 128), BF)
    pieces = pl.pallas_call(
        remote_kernel,
        out_shape=(piece,) * 4,
        in_specs=[SMEM, SMEM, SMEM, SMEM, HBM, HBM, HBM],
        out_specs=(VMEM,) * 4,
        scratch_shapes=[
            pltpu.VMEM(acc.shape, F32),
            pltpu.VMEM(acc.shape, F32),
            pltpu.VMEM((parts + 1, width, 128), BF),
            pltpu.SemaphoreType.DMA,
            pltpu.SemaphoreType.DMA,
        ]
        + ring,
        compiler_params=params(54),
        cost_estimate=cost(4 * 10**8, 20 * 2**20),
        name="remote_tiles",
    )(z, entries, ends, recv_count[0], local, far, tile_vals)

    def move(x, k):
        return lax.ppermute(x, "feat", [(i, (i + k) % 4) for i in range(4)])

    moved = [pieces[0]] + [None] * 3
    for k in (2, 1, 3):
        moved[k] = move(pieces[k], k)

    return pl.pallas_call(
        project_kernel,
        out_shape=jax.ShapeDtypeStruct((v_rows // 4, weight.shape[1]), BF),
        in_specs=[SMEM] + [VMEM] * 6,
        out_specs=VMEM,
        scratch_shapes=[pltpu.VMEM(weight.shape, BF)],
        compiler_params=params(6),
        cost_estimate=cost(3 * 10**8, 3 * 2**20),
        name="project",
    )(z, *moved, weight, bias[None, :])


def solution(mesh):
    in_specs = (
        P("feat", "vert"),
        P("vert", None, None),
        P("vert", None),
        P("vert", None),
        P("vert"),
        P("vert", None, None),
        P("vert", None),
        P(),
        P(),
    )
    out_specs = P(("vert", "feat"), None)
    return jax.shard_map(
        on_device, mesh=mesh, in_specs=in_specs, out_specs=out_specs, check_vma=False
    )
```

```python
import jax
import jax.numpy as jnp
from jax import lax
from jax.experimental import pallas as pl
from jax.experimental.pallas import tpu as pltpu
from jax.sharding import PartitionSpec as P

LOG_U = 4
U = 1 << LOG_U
LOG_V = 4
V = 1 << LOG_V
W = 4
NT = (((1,), (1,)), ((), ()))
TN = (((0,), (0,)), ((), ()))
VMEM = pl.BlockSpec(memory_space=pltpu.VMEM)
HBM = pl.BlockSpec(memory_space=pltpu.HBM)
SMEM = pl.BlockSpec(memory_space=pltpu.SMEM)
BF, F32, I32 = jnp.bfloat16, jnp.float32, jnp.int32


def params(mib):
    return pltpu.CompilerParams(vmem_limit_bytes=mib << 20)


def cost(flops, nbytes):
    return pl.CostEstimate(flops=flops, bytes_accessed=nbytes, transcendentals=0)


def prepare_kernel(
    count_ref, row_ref, col_ref, x_ref, table_ref, order_ref, list_ref, ends_ref
):
    half = table_ref.shape[0]

    def turn(k, _):
        at = pl.multiple_of(k * 128, 128)
        x = jnp.concatenate([x_ref[:, pl.ds(at, 128)], x_ref[:, pl.ds(at + half, 128)]], axis=0)
        table_ref[pl.ds(at, 128), :] = x.astype(F32).T
        return 0

    lax.fori_loop(0, half // 128, turn, 0, unroll=4)

    n = row_ref.shape[1]

    def columns(*rows):
        x = jnp.concatenate(list(rows) + [rows[0]] * (8 - len(rows)), axis=0).T
        return [x[:, k : k + 1] for k in range(len(rows))]

    def total(x):
        return jnp.sum(x, axis=1, keepdims=True)

    def count(x):
        return jnp.sum(jnp.where(x, 1.0, 0.0), axis=0, keepdims=True)

    t = lax.broadcasted_iota(I32, (1, n), 1)
    row, col = row_ref[...], col_ref[...]
    is_far = col >= 64
    used = t < count_ref[0]
    key = jnp.where(used, row + jnp.where(is_far, 64, 0), 128).astype(F32)
    (key_c,) = columns(key)
    t_c = lax.broadcasted_iota(I32, (n, 1), 0)
    less = key_c < key
    place = count((key_c == key) & (t_c < t))
    even = (place.astype(I32) & 1) == 0
    (even_c,) = columns(jnp.where(even, 1.0, 0.0))
    rank = count(less) + place
    before = jnp.sum(jnp.where(less, even_c, 0.0), axis=0, keepdims=True)
    near, far = used & ~is_far, used & is_far
    near_tiles = total(jnp.where(near, 1.0, 0.0)).astype(I32)
    used_tiles = total(jnp.where(used, 1.0, 0.0)).astype(I32)
    near_pairs = total(jnp.where(near & even, 1.0, 0.0)).astype(I32)
    far_pairs = total(jnp.where(far & even, 1.0, 0.0)).astype(I32)
    near_groups = (near_pairs + (U - 1)) >> LOG_U
    far_groups = (far_pairs + (U - 1)) >> LOG_U
    rank_i = rank.astype(I32)
    fill = jnp.where(is_far, near_groups * U - near_pairs, 0)
    slot = 2 * (before.astype(I32) + fill) + place.astype(I32)
    own = rank_i - jnp.where(is_far, near_tiles, 0)
    entry = own | (row << 9) | ((jnp.where(is_far, col - 64, col) + 1) << 15)
    rank_c, slot_c, entry_c = columns(
        jnp.where(used, rank, -1.0),
        jnp.where(used, slot, -1).astype(F32),
        jnp.where(used, entry, 0).astype(F32),
    )
    r = lax.broadcasted_iota(I32, (1, order_ref.shape[1]), 1).astype(F32)
    order = jnp.where(rank_c == r, t_c.astype(F32), 0.0)
    order_ref[...] = jnp.sum(order, axis=0, keepdims=True).astype(I32)
    s = lax.broadcasted_iota(I32, (1, list_ref.shape[1]), 1).astype(F32)
    entries = jnp.where(slot_c == s, entry_c, 0.0)
    list_ref[...] = jnp.sum(entries, axis=0, keepdims=True).astype(I32)
    lane = lax.broadcasted_iota(I32, (1, 128), 1)
    ends = jnp.where(lane == 0, near_tiles, used_tiles)
    ends = jnp.where(lane == 2, near_groups, ends)
    ends_ref[...] = jnp.where(lane == 3, far_groups, ends)


def gather_kernel(idx_ref, which_ref, table_ref, out_ref, even_ref, odd_ref, buf, sem):
    half = table_ref.shape[0]
    parts = out_ref.shape[0]

    def fill(p, rows_ref):
        own = [idx_ref.at[p + k] for k in range(W)]
        for s in range(128):
            for k in range(W):
                rows_ref[128 * k + s : 128 * k + s + 1, :] = table_ref[own[k][s] & (half - 1)]

    def turn(p, rows_ref):
        for k in range(W):
            g = rows_ref[128 * k : 128 * k + 128, :].T
            buf[p + k] = jnp.where(which_ref[p + k] < half, g[:64], g[64:]).astype(BF)

    def send(p, n):
        some = pl.ds(p, n)
        pltpu.make_async_copy(buf.at[some], out_ref.at[some], sem).start()

    def step(m, _):
        fill(2 * W * m, even_ref)
        turn(jnp.maximum(2 * W * m - W, 0), odd_ref)
        fill(2 * W * m + W, odd_ref)
        turn(2 * W * m, even_ref)

        @pl.when(m > 0)
        def _():
            send(2 * W * (m - 1), 2 * W)

        return 0

    lax.fori_loop(0, parts // (2 * W), step, 0)
    turn(parts - W, odd_ref)
    send(parts - 2 * W, 2 * W)
    pltpu.make_async_copy(buf, out_ref, sem).wait()


def bring(first, n, order_ref, vals_ref, buf, sems):
    def step(c, _):
        for k in range(V):
            i = c * V + k
            pltpu.make_async_copy(
                vals_ref.at[order_ref[0, first + i]], buf.at[i], sems.at[c]
            ).start()
        return 0

    lax.fori_loop(0, (n + (V - 1)) >> LOG_V, step, 0)


def add_pairs(first, groups, n, list_ref, block, vals_ref, buf, sems, acc_ref):
    chunks = (n + (V - 1)) >> LOG_V

    def wait(c, _):
        here = pl.ds(pl.multiple_of(c * V, V), V)
        pltpu.make_async_copy(vals_ref.at[pl.ds(0, V)], buf.at[here], sems.at[c]).wait()
        return 0

    def step(c, ready):
        at = 2 * U * (first + c)
        top = jnp.maximum(list_ref[0, at + 2 * U - 2] & 511, list_ref[0, at + 2 * U - 1] & 511)
        need = jnp.where(c == groups - 1, chunks, (top >> LOG_V) + 1)
        lax.fori_loop(ready, need, wait, 0)
        found = []
        for u in range(U):
            e, f = list_ref[0, at + 2 * u], list_ref[0, at + 2 * u + 1]
            lhs = jnp.concatenate([block(e), block(f)], axis=1)
            rhs = jnp.concatenate([buf[e & 511], buf[f & 511]], axis=1)
            found.append(
                ((e >> 9) & 63, lax.dot_general(lhs, rhs, NT, preferred_element_type=F32))
            )
        for r, product in found:
            acc_ref[r] = acc_ref[r] + product
        return need

    lax.fori_loop(0, groups, step, 0)


def local_kernel(order_ref, list_ref, ends_ref, x_ref, vals_ref, acc_ref, buf, sems):
    n = ends_ref[0, 0]
    bring(0, n, order_ref, vals_ref, buf, sems)
    acc_ref[...] = jnp.zeros_like(acc_ref)

    def block(e):
        c = jnp.maximum((e >> 15) - 1, 0)
        x = x_ref[:, pl.ds(pl.multiple_of(c * 128, 128), 128)]
        return jnp.where(e > 0, x, jnp.zeros_like(x))

    add_pairs(0, ends_ref[0, 2], n, list_ref, block, vals_ref, buf, sems, acc_ref)


def remote_kernel(
    z_ref, order_ref, list_ref, ends_ref, count_ref, sum_ref, far_ref, vals_ref, *rest
):
    out_refs, (acc_ref, sum_buf, far_buf, sum_sem, buf, sems) = rest[:4], rest[4:]
    n = ends_ref[0, 1] - ends_ref[0, 0]
    bring(ends_ref[0, 0], n, order_ref, vals_ref, buf, sems)
    sum_copy = pltpu.make_async_copy(sum_ref, sum_buf, sum_sem)
    sum_copy.start()
    acc_ref[...] = jnp.zeros_like(acc_ref)
    far_buf[0] = jnp.zeros_like(far_buf[0])
    lane = lax.broadcasted_iota(I32, far_buf.shape[1:], 1)

    def clear(q, _):
        x = far_ref[q]
        far_buf[q + 1] = jnp.where(lane < count_ref[q], x, jnp.zeros_like(x))
        return 0

    lax.fori_loop(0, far_ref.shape[0], clear, 0, unroll=4)
    add_pairs(
        ends_ref[0, 2],
        ends_ref[0, 3],
        n,
        list_ref,
        lambda e: far_buf[e >> 15],
        vals_ref,
        buf,
        sems,
        acc_ref,
    )
    sum_copy.wait()
    z = z_ref[0]
    for k, out_ref in enumerate(out_refs):
        first = ((z + k) & 3) * 16
        for r in range(16):
            out_ref[r] = (acc_ref[first + r] + sum_buf[first + r]).astype(BF)


def project_kernel(z_ref, a_ref, b_ref, c_ref, d_ref, weight_ref, bias_ref, out_ref, w_ref):
    z = z_ref[0]
    for k in range(4):
        first = pl.multiple_of(((z - k) & 3) * 64, 64)
        w_ref[64 * k : 64 * k + 64, :] = weight_ref[pl.ds(first, 64), :]
    w = w_ref[...]
    for r in range(a_ref.shape[0]):
        x = jnp.concatenate([a_ref[r], b_ref[r], c_ref[r], d_ref[r]], axis=0)
        y = lax.dot_general(x, w, TN, preferred_element_type=F32) + bias_ref[...]
        out_ref[128 * r : 128 * r + 128, :] = jnp.maximum(y, 0.0).astype(BF)


def on_device(
    features, tile_vals, tile_row, tile_col, tile_count, recv_rows, recv_count, weight, bias
):
    width, v_rows = features.shape
    parts = recv_rows.shape[1]
    wanted = lax.all_to_all(recv_rows[0], "vert", split_axis=0, concat_axis=0, tiled=True)

    n_tiles = tile_vals.shape[0]
    table, order, entries, ends = pl.pallas_call(
        prepare_kernel,
        out_shape=(
            jax.ShapeDtypeStruct((v_rows // 2, 128), F32),
            jax.ShapeDtypeStruct((1, n_tiles + 128), I32),
            jax.ShapeDtypeStruct((1, n_tiles + 128 + 128), I32),
            jax.ShapeDtypeStruct((1, 128), I32),
        ),
        in_specs=[SMEM, VMEM, VMEM, VMEM],
        out_specs=(VMEM,) * 4,
        compiler_params=params(8),
        cost_estimate=cost(10**7, 5 * 2**20),
        name="prepare",
    )(tile_count, tile_row, tile_col, features)

    outgoing = pl.pallas_call(
        gather_kernel,
        out_shape=jax.ShapeDtypeStruct((parts, width, 128), BF),
        in_specs=[SMEM, VMEM, VMEM],
        out_specs=HBM,
        scratch_shapes=[
            pltpu.VMEM((W * 128, 128), F32),
            pltpu.VMEM((W * 128, 128), F32),
            pltpu.VMEM((parts, width, 128), BF),
            pltpu.SemaphoreType.DMA,
        ],
        compiler_params=params(40),
        cost_estimate=cost(10**7, 5 * 2**20),
        name="gather",
    )(wanted, wanted.reshape(parts, 1, 128), table.reshape(v_rows // 2, 1, 128))

    far = lax.all_to_all(outgoing, "vert", split_axis=0, concat_axis=0, tiled=True)

    acc = jax.ShapeDtypeStruct((v_rows // 128, width, 128), F32)
    room = [
        pltpu.VMEM((n_tiles, 128, 128), BF),
        pltpu.SemaphoreType.DMA((n_tiles // V,)),
    ]
    local = pl.pallas_call(
        local_kernel,
        out_shape=acc,
        in_specs=[SMEM, SMEM, SMEM, VMEM, HBM],
        out_specs=VMEM,
        scratch_shapes=room,
        compiler_params=params(49),
        cost_estimate=cost(8 * 10**8, 20 * 2**20),
        name="local_tiles",
    )(order, entries, ends, features, tile_vals)

    z = lax.axis_index("feat").astype(I32)[None]
    piece = jax.ShapeDtypeStruct((16, width, 128), BF)
    pieces = pl.pallas_call(
        remote_kernel,
        out_shape=(piece,) * 4,
        in_specs=[SMEM, SMEM, SMEM, SMEM, SMEM, HBM, VMEM, HBM],
        out_specs=(VMEM,) * 4,
        scratch_shapes=[
            pltpu.VMEM(acc.shape, F32),
            pltpu.VMEM(acc.shape, F32),
            pltpu.VMEM((parts + 1, width, 128), BF),
            pltpu.SemaphoreType.DMA,
        ]
        + room,
        compiler_params=params(49),
        cost_estimate=cost(4 * 10**8, 20 * 2**20),
        name="remote_tiles",
    )(z, order, entries, ends, recv_count[0], local, far, tile_vals)

    def move(x, k):
        return lax.ppermute(x, "feat", [(i, (i + k) % 4) for i in range(4)])

    moved = [pieces[0]] + [None] * 3
    for k in (2, 1, 3):
        moved[k] = move(pieces[k], k)

    return pl.pallas_call(
        project_kernel,
        out_shape=jax.ShapeDtypeStruct((v_rows // 4, weight.shape[1]), BF),
        in_specs=[SMEM] + [VMEM] * 6,
        out_specs=VMEM,
        scratch_shapes=[pltpu.VMEM(weight.shape, BF)],
        compiler_params=params(6),
        cost_estimate=cost(3 * 10**8, 3 * 2**20),
        name="project",
    )(z, *moved, weight, bias[None, :])


def solution(mesh):
    in_specs = (
        P("feat", "vert"),
        P("vert", None, None),
        P("vert", None),
        P("vert", None),
        P("vert"),
        P("vert", None, None),
        P("vert", None),
        P(),
        P(),
    )
    out_specs = P(("vert", "feat"), None)
    return jax.shard_map(
        on_device, mesh=mesh, in_specs=in_specs, out_specs=out_specs, check_vma=False
    )
```

```python
import functools

import jax
import jax.numpy as jnp
from jax import lax
from jax.experimental import pallas as pl
from jax.experimental.pallas import tpu as pltpu
from jax.sharding import PartitionSpec as P

NEAR = 5
FAR = 4
LOG_V = 4
V = 1 << LOG_V
W = 4
NT = (((1,), (1,)), ((), ()))
TN = (((0,), (0,)), ((), ()))
VMEM = pl.BlockSpec(memory_space=pltpu.VMEM)
HBM = pl.BlockSpec(memory_space=pltpu.HBM)
SMEM = pl.BlockSpec(memory_space=pltpu.SMEM)
BF, F32, I32 = jnp.bfloat16, jnp.float32, jnp.int32


def params(mib):
    return pltpu.CompilerParams(vmem_limit_bytes=mib << 20)


def cost(flops, nbytes):
    return pl.CostEstimate(flops=flops, bytes_accessed=nbytes, transcendentals=0)


def prepare_kernel(
    count_ref, row_ref, col_ref, x_ref, table_ref, order_ref, list_ref, ends_ref
):
    half = table_ref.shape[0]

    def turn(k, _):
        at = pl.multiple_of(k * 128, 128)
        x = jnp.concatenate([x_ref[:, pl.ds(at, 128)], x_ref[:, pl.ds(at + half, 128)]], axis=0)
        table_ref[pl.ds(at, 128), :] = x.astype(F32).T
        return 0

    lax.fori_loop(0, half // 128, turn, 0, unroll=4)

    n = row_ref.shape[1]

    def columns(*rows):
        x = jnp.concatenate(list(rows) + [rows[0]] * (8 - len(rows)), axis=0).T
        return [x[:, k : k + 1] for k in range(len(rows))]

    def total(x):
        return jnp.sum(x, axis=1, keepdims=True)

    def count(x):
        return jnp.sum(jnp.where(x, 1.0, 0.0), axis=0, keepdims=True)

    t = lax.broadcasted_iota(I32, (1, n), 1)
    row, col = row_ref[...], col_ref[...]
    is_far = col >= 64
    used = t < count_ref[0]
    key = jnp.where(used, row + jnp.where(is_far, 64, 0), 128).astype(F32)
    (key_c,) = columns(key)
    t_c = lax.broadcasted_iota(I32, (n, 1), 0)
    less = key_c < key
    place = count((key_c == key) & (t_c < t))
    even = (place.astype(I32) & 1) == 0
    (even_c,) = columns(jnp.where(even, 1.0, 0.0))
    rank = count(less) + place
    before = jnp.sum(jnp.where(less, even_c, 0.0), axis=0, keepdims=True)
    part = jnp.where(is_far, 1 + (row >> 4), 0)
    tiles, groups, first_tile, first_group = [], [], [], []
    tile_at = pair_at = row[:, :1] * 0
    filled = row[:, :1] * 0
    fill = row * 0
    own = rank.astype(I32)
    for k in range(5):
        here = used & (part == k)
        unit = NEAR if k == 0 else FAR
        k_tiles = total(jnp.where(here, 1.0, 0.0)).astype(I32)
        k_pairs = total(jnp.where(here & even, 1.0, 0.0)).astype(I32)
        k_groups = (k_pairs + ((1 << unit) - 1)) >> unit
        fill = jnp.where(part == k, filled, fill)
        own = jnp.where(part == k, own - tile_at, own)
        first_tile.append(tile_at)
        first_group.append((pair_at + filled) >> FAR)
        tiles.append(k_tiles)
        groups.append(k_groups)
        tile_at = tile_at + k_tiles
        pair_at = pair_at + k_pairs
        filled = filled + (k_groups << unit) - k_pairs
    slot = 2 * (before.astype(I32) + fill) + place.astype(I32)
    entry = own | (row << 9) | ((jnp.where(is_far, col - 64, col) + 1) << 15)
    rank_c, slot_c, entry_c = columns(
        jnp.where(used, rank, -1.0),
        jnp.where(used, slot, -1).astype(F32),
        jnp.where(used, entry, 0).astype(F32),
    )
    r = lax.broadcasted_iota(I32, (1, order_ref.shape[1]), 1).astype(F32)
    order = jnp.where(rank_c == r, t_c.astype(F32), 0.0)
    order_ref[...] = jnp.sum(order, axis=0, keepdims=True).astype(I32)
    s = lax.broadcasted_iota(I32, (1, list_ref.shape[1]), 1).astype(F32)
    entries = jnp.where(slot_c == s, entry_c, 0.0)
    list_ref[...] = jnp.sum(entries, axis=0, keepdims=True).astype(I32)
    lane = lax.broadcasted_iota(I32, (1, 128), 1)
    ends = lane * 0
    for k in range(5):
        for i, x in enumerate((first_tile[k], tiles[k], first_group[k], groups[k])):
            ends = jnp.where(lane == 4 * k + i, x, ends)
    ends_ref[...] = ends


def gather_kernel(idx_ref, which_ref, table_ref, out_ref, even_ref, odd_ref, buf, sem):
    half = table_ref.shape[0]
    parts = out_ref.shape[0]

    def fill(p, rows_ref):
        own = [idx_ref.at[p + k] for k in range(W)]
        for s in range(128):
            for k in range(W):
                rows_ref[128 * k + s : 128 * k + s + 1, :] = table_ref[own[k][s] & (half - 1)]

    def turn(p, rows_ref):
        for k in range(W):
            g = rows_ref[128 * k : 128 * k + 128, :].T
            buf[p + k] = jnp.where(which_ref[p + k] < half, g[:64], g[64:]).astype(BF)

    def send(p, n):
        some = pl.ds(p, n)
        pltpu.make_async_copy(buf.at[some], out_ref.at[some], sem).start()

    def step(m, _):
        fill(2 * W * m, even_ref)
        turn(jnp.maximum(2 * W * m - W, 0), odd_ref)
        fill(2 * W * m + W, odd_ref)
        turn(2 * W * m, even_ref)

        @pl.when(m > 0)
        def _():
            send(2 * W * (m - 1), 2 * W)

        return 0

    lax.fori_loop(0, parts // (2 * W), step, 0)
    turn(parts - W, odd_ref)
    send(parts - 2 * W, 2 * W)
    pltpu.make_async_copy(buf, out_ref, sem).wait()


def bring(part, order_ref, ends_ref, vals_ref, buf, sems, base=0):
    first, n = ends_ref[0, 4 * part], ends_ref[0, 4 * part + 1]

    def step(c, _):
        for k in range(V):
            i = c * V + k
            pltpu.make_async_copy(
                vals_ref.at[order_ref[0, first + i]], buf.at[base * V + i], sems.at[base + c]
            ).start()
        return 0

    chunks = (n + (V - 1)) >> LOG_V
    lax.fori_loop(0, chunks, step, 0)
    return chunks


def add_pairs(part, unit, list_ref, ends_ref, block, vals_ref, buf, sems, acc_ref, base=0):
    n, first, groups = (ends_ref[0, 4 * part + i] for i in (1, 2, 3))
    chunks = (n + (V - 1)) >> LOG_V
    size = 1 << unit
    offset = base * V

    def wait(c, _):
        here = pl.ds(pl.multiple_of((base + c) * V, V), V)
        pltpu.make_async_copy(vals_ref.at[pl.ds(0, V)], buf.at[here], sems.at[base + c]).wait()
        return 0

    def step(c, ready):
        at = (first << (FAR + 1)) + 2 * size * c
        top = jnp.maximum(
            list_ref[0, at + 2 * size - 2] & 511, list_ref[0, at + 2 * size - 1] & 511
        )
        need = jnp.where(c == groups - 1, chunks, (top >> LOG_V) + 1)
        lax.fori_loop(ready, need, wait, 0)
        found = []
        for u in range(size):
            e, f = list_ref[0, at + 2 * u], list_ref[0, at + 2 * u + 1]
            lhs = jnp.concatenate([block(e), block(f)], axis=1)
            rhs = jnp.concatenate([buf[offset + (e & 511)], buf[offset + (f & 511)]], axis=1)
            product = lax.dot_general(lhs, rhs, NT, preferred_element_type=F32)
            found.append(((e >> 9) & (acc_ref.shape[0] - 1), product))
        for r, product in found:
            acc_ref[r] = acc_ref[r] + product
        return need

    lax.fori_loop(0, groups, step, 0)


def local_kernel(order_ref, list_ref, ends_ref, x_ref, vals_ref, acc_ref, buf, sems):
    bring(0, order_ref, ends_ref, vals_ref, buf, sems)
    acc_ref[...] = jnp.zeros_like(acc_ref)

    def block(e):
        c = jnp.maximum((e >> 15) - 1, 0)
        x = x_ref[:, pl.ds(pl.multiple_of(c * 128, 128), 128)]
        return jnp.where(e > 0, x, jnp.zeros_like(x))

    add_pairs(0, NEAR, list_ref, ends_ref, block, vals_ref, buf, sems, acc_ref)


def clear(count_ref, far_ref, out_ref):
    out_ref[0] = jnp.zeros_like(out_ref[0])
    lane = lax.broadcasted_iota(I32, far_ref.shape[1:], 1)

    def step(q, _):
        x = far_ref[q]
        out_ref[q + 1] = jnp.where(lane < count_ref[q], x, jnp.zeros_like(x))
        return 0

    lax.fori_loop(0, far_ref.shape[0], step, 0, unroll=4)


def remote_kernel(shifts, *refs):
    z_ref, order_ref, list_ref, ends_ref, sum_ref, vals_ref = refs[:6]
    refs = refs[6:]
    if shifts[0] == 2:
        count_ref, raw_ref, out_ref, far_ref, acc_ref, buf, sems = refs
        out_refs = [out_ref]
    else:
        far_ref = refs[0]
        out_refs = refs[1 : 1 + len(shifts)]
        acc_ref, buf, sems = refs[1 + len(shifts) :]
    z = z_ref[0]
    base, bases = 0, []
    for k in shifts:
        bases.append(base)
        base += bring(1 + ((z + k) & 3), order_ref, ends_ref, vals_ref, buf, sems, base)
    for i, k in enumerate(shifts):
        for r in range(16):
            acc_ref[i, r] = sum_ref[((z + k) & 3) * 16 + r]
    if shifts[0] == 2:
        clear(count_ref, raw_ref, far_ref)
    for i, k in enumerate(shifts):
        part = 1 + ((z + k) & 3)
        block = lambda e: far_ref[e >> 15]
        add_pairs(
            part, FAR, list_ref, ends_ref, block, vals_ref, buf, sems, acc_ref.at[i], bases[i]
        )
        for r in range(16):
            out_refs[i][r] = acc_ref[i, r].astype(BF)


def project_kernel(
    z_ref, a_ref, b_ref, c_ref, d_ref, weight_ref, bias_ref, out_ref, w_ref, buf, sem
):
    z = z_ref[0]
    for k in range(4):
        first = pl.multiple_of(((z - k) & 3) * 64, 64)
        w_ref[64 * k : 64 * k + 64, :] = weight_ref[pl.ds(first, 64), :]
    w = w_ref[...]
    n = a_ref.shape[0]
    for r in range(n):
        x = jnp.concatenate([a_ref[r], b_ref[r], c_ref[r], d_ref[r]], axis=0)
        y = lax.dot_general(x, w, TN, preferred_element_type=F32) + bias_ref[...]
        buf[128 * r : 128 * r + 128, :] = jnp.maximum(y, 0.0).astype(BF)
        if r % 4 == 3:
            here = pl.ds(128 * (r - 3), 512)
            pltpu.make_async_copy(buf.at[here], out_ref.at[here], sem).start()
    pltpu.make_async_copy(buf, out_ref, sem).wait()


def on_device(
    features, tile_vals, tile_row, tile_col, tile_count, recv_rows, recv_count, weight, bias
):
    width, v_rows = features.shape
    parts = recv_rows.shape[1]
    wanted = lax.all_to_all(recv_rows[0], "vert", split_axis=0, concat_axis=0, tiled=True)

    n_tiles = tile_vals.shape[0]
    table, order, entries, ends = pl.pallas_call(
        prepare_kernel,
        out_shape=(
            jax.ShapeDtypeStruct((v_rows // 2, 128), F32),
            jax.ShapeDtypeStruct((1, n_tiles + 128), I32),
            jax.ShapeDtypeStruct((1, n_tiles + 384), I32),
            jax.ShapeDtypeStruct((1, 128), I32),
        ),
        in_specs=[SMEM, VMEM, VMEM, VMEM],
        out_specs=(VMEM,) * 4,
        compiler_params=params(8),
        cost_estimate=cost(10**7, 5 * 2**20),
        name="prepare",
    )(tile_count, tile_row, tile_col, features)

    outgoing = pl.pallas_call(
        gather_kernel,
        out_shape=pltpu.HBM((parts, width, 128), BF),
        in_specs=[SMEM, VMEM, VMEM],
        out_specs=HBM,
        scratch_shapes=[
            pltpu.VMEM((W * 128, 128), F32),
            pltpu.VMEM((W * 128, 128), F32),
            pltpu.VMEM((parts, width, 128), BF),
            pltpu.SemaphoreType.DMA,
        ],
        compiler_params=params(40),
        cost_estimate=cost(10**7, 5 * 2**20),
        name="gather",
    )(wanted, wanted.reshape(parts, 1, 128), table.reshape(v_rows // 2, 1, 128))

    far = lax.all_to_all(outgoing, "vert", split_axis=0, concat_axis=0, tiled=True)

    acc = jax.ShapeDtypeStruct((v_rows // 128, width, 128), F32)
    room = [
        pltpu.VMEM((n_tiles, 128, 128), BF),
        pltpu.SemaphoreType.DMA((n_tiles // V,)),
    ]
    local = pl.pallas_call(
        local_kernel,
        out_shape=acc,
        in_specs=[SMEM, SMEM, SMEM, VMEM, HBM],
        out_specs=VMEM,
        scratch_shapes=room,
        compiler_params=params(49),
        cost_estimate=cost(8 * 10**8, 20 * 2**20),
        name="local_tiles",
    )(order, entries, ends, features, tile_vals)

    z = lax.axis_index("feat").astype(I32)[None]
    piece = jax.ShapeDtypeStruct((16, width, 128), BF)
    far_shape = jax.ShapeDtypeStruct((parts + 1, width, 128), BF)

    def remote(shifts, *more):
        first = shifts[0] == 2
        n = len(shifts)
        rows = n_tiles + V * (n - 1)
        out = pl.pallas_call(
            functools.partial(remote_kernel, shifts),
            out_shape=(piece,) * n + ((far_shape,) if first else ()),
            in_specs=[SMEM] * 4 + [VMEM, HBM] + ([SMEM, VMEM] if first else [VMEM]),
            out_specs=(VMEM,) * (n + first),
            scratch_shapes=[
                pltpu.VMEM((n, 16, width, 128), F32),
                pltpu.VMEM((rows, 128, 128), BF),
                pltpu.SemaphoreType.DMA((rows // V,)),
            ],
            compiler_params=params(49),
            cost_estimate=cost(n * 10**8, 5 * n * 2**20),
            name="remote_tiles_" + "".join(str(k) for k in shifts),
        )(z, order, entries, ends, local, tile_vals, *more)
        return out

    def move(x, k):
        return lax.ppermute(x, "feat", [(i, (i + k) % 4) for i in range(4)])

    moved = [None] * 4
    out, far = remote((2,), recv_count[0], far)
    moved[2] = move(out, 2)
    out = remote((1, 3), far)
    moved[1], moved[3] = move(out[0], 1), move(out[1], 3)
    (moved[0],) = remote((0,), far)

    return pl.pallas_call(
        project_kernel,
        out_shape=jax.ShapeDtypeStruct((v_rows // 4, weight.shape[1]), BF),
        in_specs=[SMEM] + [VMEM] * 6,
        out_specs=HBM,
        scratch_shapes=[
            pltpu.VMEM(weight.shape, BF),
            pltpu.VMEM((v_rows // 4, weight.shape[1]), BF),
            pltpu.SemaphoreType.DMA,
        ],
        compiler_params=params(6),
        cost_estimate=cost(3 * 10**8, 3 * 2**20),
        name="project",
    )(z, *moved, weight, bias[None, :])


def solution(mesh):
    in_specs = (
        P("feat", "vert"),
        P("vert", None, None),
        P("vert", None),
        P("vert", None),
        P("vert"),
        P("vert", None, None),
        P("vert", None),
        P(),
        P(),
    )
    out_specs = P(("vert", "feat"), None)
    return jax.shard_map(
        on_device, mesh=mesh, in_specs=in_specs, out_specs=out_specs, check_vma=False
    )
```
